32 devices in a mesh: gx: 4 (over x, core), gy: 4 (over z), gz: 2 (over y).
Axes of the slice: x: 2, y: 2, z: 4, core: 2. Of those that a mesh axis runs over, the one named last changes fastest.
Arguments:
- velocity: float32 [3, 32, 128, 512], P(None, 'gz', 'gy', 'gx'), may hold values from -14 to 14, as said below
- geometry: bfloat16 [6, 32, 128, 512], P(None, 'gz', 'gy', 'gx'), may hold values from -0.015 to 0.041, as said below
- mass_weights: bfloat16 [32, 128, 512], P('gz', 'gy', 'gx'), may hold values from 0.0099487305 to 0.099609375
Outputs:
- residual: float32 [3, 32, 128, 512], P(None, 'gz', 'gy', 'gx')
- kinetic: float32 [], replicated
- enstrophy: float32 [], replicated
The draws below stay inside these ranges and needn't reach their ends.
Inputs may be any that keep to these rules, and one draw needn't show every extreme that they name: `velocity`: coincident points of neighbouring elements hold equal values, and points on the outer boundary of the grid hold zero. `geometry`: at every point the matrix [[g0, g3, g4], [g3, g1, g5], [g4, g5, g2]] is positive definite.
All inputs are finite; a program needn't handle non-finite values.
Results may differ from the reference program's by a relative error of at most 0.0003.
Values sent between devices are 32-bit elements; how exact they have to be, the bound alone decides.
A program may use at most 128 MiB of HBM per device.

```python
import math
import jax
import jax.numpy as jnp
import numpy as np
from jax import lax

ORDER = 7
POINTS = 8
GX = 512
GY = 128
GZ = 32


def join_faces(source, which_dim):
    position = lax.broadcasted_iota(jnp.int32, source.shape, which_dim)
    prev_val = jnp.roll(source, 1, which_dim)
    return jnp.where((position % (ORDER + 1) == 0) & (position > 0), prev_val, source)


def ramp_along(extent, which_dim):
    position = lax.broadcasted_iota(jnp.int32, extent, which_dim).astype(jnp.float32)
    return 0.5 + position / (extent[which_dim] - 1)


def draw_velocity(key, part):
    extent = (GZ, GY, GX)
    ramp_total = ramp_along(extent, 0) * ramp_along(extent, 1) * ramp_along(extent, 2)

    def one_component(comp_id):
        subkey = jax.random.fold_in(key, comp_id)
        noise = jnp.clip(jax.random.normal(subkey, extent, jnp.float32), -4.0, 4.0)
        field_now = noise * ramp_total
        field_now = join_faces(join_faces(join_faces(field_now, 2), 1), 0)
        inside = jnp.ones(extent, dtype=bool)
        for which_dim in range(3):
            position = lax.broadcasted_iota(jnp.int32, extent, which_dim)
            inside = inside & (position > 0) & (position < extent[which_dim] - 1)
        return jnp.where(inside, field_now, 0.0)
    return lax.map(one_component, jnp.arange(3)).astype(jnp.float32)


def draw_geometry(key, part):
    extent = (GZ, GY, GX)
    keyset = jax.random.split(key, 6)
    bottom, upper_end, reach = (0.003, 0.03, 0.3)
    diagonal = []
    for slot_id in range(3):
        drawn = jax.random.uniform(keyset[slot_id], extent, jnp.float32, math.log(bottom), math.log(upper_end))
        diagonal.append(jnp.exp(drawn))
    pairs_list = ((0, 1), (0, 2), (1, 2))
    offdiag = []
    for slot_id in range(3):
        first_id, second_id = pairs_list[slot_id]
        factor = jax.random.uniform(keyset[3 + slot_id], extent, jnp.float32, -reach, reach)
        offdiag.append(factor * jnp.sqrt(diagonal[first_id] * diagonal[second_id]))
    return jnp.stack(diagonal + offdiag, 0).astype(jnp.bfloat16)


def level_of(rng, shape, cuts, low, largest):
    level = 1.0
    for dim, shards_of in cuts:
        draws = jax.random.uniform(jax.random.fold_in(jax.random.fold_in(rng, 6), dim), (shards_of,), jnp.float32, low / len(cuts), largest / len(cuts))
        level = level * jnp.repeat(jnp.exp(draws), shape[dim] // shards_of).reshape((-1,) + (1,) * (len(shape) - 1 - dim))
    return level


def setup_inputs(seed: int = 0) -> dict:
    key_list = jax.random.split(jax.random.key(seed), 4)
    return {
        "velocity": draw_velocity(jax.random.fold_in(key_list[3], 71), 0),
        "geometry": draw_geometry(jax.random.fold_in(key_list[3], 71), 0),
        "mass_weights": jnp.clip(jnp.exp(math.log(0.099609375) - 2.3038113 * jax.random.uniform(key_list[2], (GZ, GY, GX), jnp.float32) ** level_of(key_list[2], (GZ, GY, GX), ((0, 2), (1, 4), (2, 4)), -0.2, 0.2)), 0.0099487305, 0.099609375).astype(jnp.bfloat16),
    }


def gll_derivative(poly_order):
    node_count = poly_order + 1
    abscissa = np.cos(np.pi * np.arange(node_count) / poly_order)
    legendre = np.zeros((node_count, node_count))
    for newton_step in range(60):
        legendre[:, 0] = 1.0
        legendre[:, 1] = abscissa
        for degree in range(2, node_count):
            legendre[:, degree] = ((2 * degree - 1) * abscissa * legendre[:, degree - 1] - (degree - 1) * legendre[:, degree - 2]) / degree
        abscissa = abscissa - (abscissa * legendre[:, poly_order] - legendre[:, poly_order - 1]) / (node_count * legendre[:, poly_order])
    abscissa = abscissa[::-1]
    end_values = legendre[::-1, poly_order]
    spacing = abscissa[:, None] - abscissa[None, :] + np.eye(node_count)
    deriv_table = end_values[:, None] / end_values[None, :] / spacing
    deriv_table = deriv_table * (1.0 - np.eye(node_count))
    deriv_table[0, 0] = -poly_order * node_count / 4.0
    deriv_table[poly_order, poly_order] = poly_order * node_count / 4.0
    return deriv_table.astype(np.float32)


def derive(source, matrix, which_dim):
    highest = lax.Precision.HIGHEST
    points = matrix.shape[0]
    extent = source.shape
    split_shape = extent[:which_dim] + (extent[which_dim] // points, points) + extent[which_dim + 1:]
    pieces = source.reshape(split_shape)
    if which_dim == 3:
        result = jnp.einsum('czyex,wx->czyew', pieces, matrix, precision=highest)
    elif which_dim == 2:
        result = jnp.einsum('czeyx,wy->czewx', pieces, matrix, precision=highest)
    else:
        result = jnp.einsum('cezyx,wz->cewyx', pieces, matrix, precision=highest)
    return result.reshape(extent)


def metric(geometry, slot_id):
    return geometry[slot_id].astype(jnp.float32)[None]


def apply_local(velocity, geometry, matrix):
    grad_r = derive(velocity, matrix, 3)
    grad_s = derive(velocity, matrix, 2)
    grad_t = derive(velocity, matrix, 1)
    flux_r = metric(geometry, 0) * grad_r + metric(geometry, 3) * grad_s + metric(geometry, 4) * grad_t
    flux_s = metric(geometry, 3) * grad_r + metric(geometry, 1) * grad_s + metric(geometry, 5) * grad_t
    flux_t = metric(geometry, 4) * grad_r + metric(geometry, 5) * grad_s + metric(geometry, 2) * grad_t
    enstrophy_part = jnp.sum(grad_r * flux_r + grad_s * flux_s + grad_t * flux_t)
    transposed = matrix.T
    applied = derive(flux_r, transposed, 3) + derive(flux_s, transposed, 2) + derive(flux_t, transposed, 1)
    return applied, enstrophy_part


def assemble_axis(source, which_dim):
    length = source.shape[which_dim]
    position = lax.broadcasted_iota(jnp.int32, source.shape, which_dim)
    next_val = jnp.roll(source, -1, which_dim)
    prev_val = jnp.roll(source, 1, which_dim)
    up_mask = (position % POINTS == POINTS - 1) & (position < length - 1)
    low_mask = (position % POINTS == 0) & (position > 0)
    return source + jnp.where(up_mask, next_val, 0.0) + jnp.where(low_mask, prev_val, 0.0)


def assemble_one(single_field):
    return assemble_axis(assemble_axis(assemble_axis(single_field, 2), 1), 0)


def reference(velocity, geometry, mass_weights):
    matrix = jnp.asarray(gll_derivative(ORDER), jnp.float32)
    mass_float = mass_weights.astype(jnp.float32)
    kinetic = 0.5 * jnp.sum(mass_float[None] * velocity * velocity)
    layers = velocity.shape[1] // POINTS

    def layer_step(layer_id, state_pair):
        applied, energy = state_pair
        offset = (layer_id * POINTS).astype(jnp.int32)
        block_vel = lax.dynamic_slice_in_dim(velocity, offset, POINTS, 1)
        block_geo = lax.dynamic_slice_in_dim(geometry, offset, POINTS, 1)
        part_field, part_energy = apply_local(block_vel, block_geo, matrix)
        applied = lax.dynamic_update_slice_in_dim(applied, part_field, offset, 1)
        return applied, energy + part_energy

    start_pair = (jnp.zeros(velocity.shape, jnp.float32), jnp.zeros((), jnp.float32))
    applied, enstrophy = lax.fori_loop(0, layers, layer_step, start_pair)
    stacked = jnp.concatenate([applied, mass_float[None]], 0)
    assembled = lax.map(assemble_one, stacked)
    extent = velocity.shape[1:]
    interior = jnp.ones(extent, dtype=bool)
    for which_dim in range(3):
        position = lax.broadcasted_iota(jnp.int32, extent, which_dim)
        interior = interior & (position > 0) & (position < extent[which_dim] - 1)
    rayleigh = enstrophy / (2.0 * kinetic)
    residual = jnp.where(interior[None], assembled[:3] - rayleigh * assembled[3][None] * velocity, 0.0)
    return residual, kinetic, enstrophy
```

```python
import functools
import itertools

import jax
import jax.numpy as jnp
import numpy as np
from jax import lax
from jax.experimental import pallas as pl
from jax.experimental.pallas import tpu as pltpu
from jax.sharding import PartitionSpec as P

ORDER = 7
PTS = ORDER + 1
MESH = pl.DeviceIdType.MESH
AXES = ("gx", "gy", "gz")
XOFF = [o for o in itertools.product((-1, 0, 1), repeat=3) if o[0] != 0]
YZOFF = [o for o in itertools.product((-1, 0, 1), repeat=3) if o[0] == 0 and o[1] != 0 and o[2] != 0]
YOFF = [(0, -1, 0), (0, 1, 0)]
ZOFF = [(0, 0, -1), (0, 0, 1)]
OFFS = sorted(XOFF + YZOFF + YOFF + ZOFF, key=lambda o: -sum(map(abs, o)))


def gll_derivative(poly_order):
    node_count = poly_order + 1
    abscissa = np.cos(np.pi * np.arange(node_count) / poly_order)
    legendre = np.zeros((node_count, node_count))
    for newton_step in range(60):
        legendre[:, 0] = 1.0
        legendre[:, 1] = abscissa
        for degree in range(2, node_count):
            legendre[:, degree] = (
                (2 * degree - 1) * abscissa * legendre[:, degree - 1]
                - (degree - 1) * legendre[:, degree - 2]
            ) / degree
        abscissa = abscissa - (abscissa * legendre[:, poly_order] - legendre[:, poly_order - 1]) / (
            node_count * legendre[:, poly_order]
        )
    abscissa = abscissa[::-1]
    end_values = legendre[::-1, poly_order]
    spacing = abscissa[:, None] - abscissa[None, :] + np.eye(node_count)
    deriv_table = end_values[:, None] / end_values[None, :] / spacing
    deriv_table = deriv_table * (1.0 - np.eye(node_count))
    deriv_table[0, 0] = -poly_order * node_count / 4.0
    deriv_table[poly_order, poly_order] = poly_order * node_count / 4.0
    return deriv_table.astype(np.float32)


def split_np(m):
    hi = m.astype(jnp.bfloat16)
    lo = (m - hi.astype(np.float32)).astype(jnp.bfloat16)
    return hi, lo


def tables(rows, cols):
    d = gll_derivative(ORDER)
    out = []
    for mat in (d, d.T):
        hi, lo = split_np(np.kron(np.eye(cols // PTS, dtype=np.float32), mat.T))
        zero = np.zeros_like(lo)
        out.append(np.block([[hi, lo], [hi, zero]]))
        hi, lo = split_np(np.kron(np.eye(PTS * rows // PTS, dtype=np.float32), mat))
        out.append(np.stack([hi, lo]))
    pick = np.zeros((2 * cols, 2 * cols), np.float32)
    for base in (0, cols):
        pick[base, :cols] = 1.0
        pick[base + cols - 1, cols:] = 1.0
    out.append(pick.astype(jnp.bfloat16))
    put = np.zeros((2 * cols, cols), np.float32)
    put[:cols, cols - 1] = 1.0
    put[cols:, 0] = 1.0
    out.append(put.astype(jnp.bfloat16))
    return [jnp.asarray(t) for t in out]


def split(x):
    hi = x.astype(jnp.bfloat16)
    lo = (x - hi.astype(jnp.float32)).astype(jnp.bfloat16)
    return hi, lo


def dot(a, b):
    return jnp.dot(a, b, preferred_element_type=jnp.float32)


def along_x(pair, table):
    cols = table.shape[1] // 2
    r = dot(jnp.concatenate(pair, axis=1), table)
    return r[:, :cols] + r[:, cols:]


def along_y(pair, hi, lo):
    cols = pair[0].shape[1]
    r = dot(hi, jnp.concatenate(pair, axis=1))
    return r[:, :cols] + r[:, cols:] + dot(lo, pair[0])


def along_z(planes, mat):
    out = []
    for w in range(PTS):
        acc = planes[0] * float(mat[w, 0])
        for z in range(1, PTS):
            acc = acc + planes[z] * float(mat[w, z])
        out.append(acc)
    return out


def kernel(
    sizes,
    v_hbm, g_hbm, m_hbm, dx_ref, dy_ref, tx_ref, ty_ref, pick_ref, put_ref,
    a_out, m_out, s_out,
    v, g, m, flux, field, pack, yface, yzrow, rpack, ryface, rzface, ryz, part, parts,
    in_sem, send_sem, recv_sem, ssend, srecv,
):
    nx, ny, nz = sizes
    count = nx * ny * nz
    planes, rows, cols = v.shape[1:]
    layers = planes // PTS
    yel = rows // PTS
    half = cols // 2
    ix, iy, iz = (lax.axis_index(a) for a in AXES)
    me = (ix * ny + iy) * nz + iz
    d = gll_derivative(ORDER)

    loads = [
        pltpu.make_async_copy(src, dst, in_sem.at[k])
        for k, (src, dst) in enumerate(((m_hbm, m), (v_hbm, v), (g_hbm, g)))
    ]
    for c in loads:
        c.start()

    def peer_id(step):
        p = lax.rem(me + step, count)
        return {"gx": p // (ny * nz), "gy": lax.rem(p // nz, ny), "gz": lax.rem(p, nz)}

    barrier = pltpu.get_barrier_semaphore()

    @pl.loop(1, count)
    def _(step):
        pl.semaphore_signal(barrier, inc=1, device_id=peer_id(step), device_id_type=MESH)

    four = (PTS, yel, PTS, cols)
    ye_at = lax.broadcasted_iota(jnp.int32, four, 1)
    k_at = lax.broadcasted_iota(jnp.int32, four, 2)
    z_at = lax.broadcasted_iota(jnp.int32, four, 0)
    lane = lax.broadcasted_iota(jnp.int32, four, 3)
    lane2 = lax.broadcasted_iota(jnp.int32, (PTS * rows, cols), 1)
    row2 = lax.broadcasted_iota(jnp.int32, (PTS * rows, cols), 0)

    def assemble_xy(x):
        n = PTS * rows
        x = (
            x
            + jnp.where((lane2 % PTS == ORDER) & (lane2 < cols - 1), pltpu.roll(x, cols - 1, 1), 0.0)
            + jnp.where((lane2 % PTS == 0) & (lane2 > 0), pltpu.roll(x, 1, 1), 0.0)
        )
        return (
            x
            + jnp.where((row2 % PTS == ORDER) & (row2 % rows < rows - 1), pltpu.roll(x, n - 1, 0), 0.0)
            + jnp.where((row2 % PTS == 0) & (row2 % rows > 0), pltpu.roll(x, 1, 0), 0.0)
        )

    def finish_channel(c):
        for e in range(1, layers):
            low = field[c, e * PTS - 1]
            high = field[c, e * PTS]
            both = low + high
            field[c, e * PTS - 1] = both
            field[c, e * PTS] = both
        lo_acc = jnp.zeros((PTS, cols), jnp.float32)
        hi_acc = jnp.zeros((PTS, cols), jnp.float32)
        base = (c % 2) * half
        for e in range(layers):
            x = field[c, pl.ds(e * PTS, PTS)].reshape(PTS * rows, cols)
            r = dot(jnp.concatenate(split(x), axis=1), pick_ref[...])
            hit = lane == base + (e * PTS + z_at) * yel + ye_at
            lo_acc = lo_acc + jnp.sum(jnp.where(hit, r[:, :cols].reshape(four), 0.0), axis=(0, 1))
            hi_acc = hi_acc + jnp.sum(jnp.where(hit, r[:, cols:].reshape(four), 0.0), axis=(0, 1))
        pair = c // 2
        pack[0, pair] = pack[0, pair] + lo_acc
        pack[1, pair] = pack[1, pair] + hi_acc
        for side, y in ((0, 0), (1, rows - 1)):
            face = field[c, :, y, :]
            yface[side, c] = face
            yzrow[side, 0, c] = face[0:1]
            yzrow[side, 1, c] = face[planes - 1:planes]

    pack[...] = jnp.zeros(pack.shape, jnp.float32)
    loads[0].wait()
    for e in range(layers):
        x = m[pl.ds(e * PTS, PTS)].astype(jnp.float32).reshape(PTS * rows, cols)
        field[3, pl.ds(e * PTS, PTS)] = assemble_xy(x).reshape(PTS, rows, cols)
    finish_channel(3)
    loads[1].wait()
    loads[2].wait()

    def gradients(step, acc):
        kin, ens = acc
        c = step // layers
        at = pl.ds(pl.multiple_of((step % layers) * PTS, PTS), PTS)
        block = v[c, at]
        flat = block.reshape(PTS * rows, cols)
        mass = m[at].astype(jnp.float32)
        kin = kin + jnp.sum((mass * block * block).reshape(-1, PTS, cols), axis=0)
        pair = split(flat)
        gr = along_x(pair, dx_ref[...]).reshape(block.shape)
        gs = along_y(pair, dy_ref[0], dy_ref[1]).reshape(block.shape)
        gt = jnp.stack(along_z([block[z] for z in range(PTS)], d))
        g0, g1, g2, g3, g4, g5 = (g[k, at].astype(jnp.float32) for k in range(6))
        fr = g0 * gr + g3 * gs + g4 * gt
        fs = g3 * gr + g1 * gs + g5 * gt
        ft = g4 * gr + g5 * gs + g2 * gt
        ens = ens + jnp.sum((gr * fr + gs * fs + gt * ft).reshape(-1, PTS, cols), axis=0)
        flux[0, c, at] = fr
        flux[1, c, at] = fs
        flux[2, c, at] = ft
        return kin, ens

    zero = jnp.zeros((PTS, cols), jnp.float32)
    kin, ens = lax.fori_loop(0, 3 * layers, gradients, (zero, zero))
    mine = jnp.concatenate(
        [jnp.sum(kin, 0, keepdims=True) * 0.5, jnp.sum(ens, 0, keepdims=True)], axis=0
    )
    part[...] = mine
    parts[me] = mine

    pl.semaphore_wait(barrier, count - 1)

    def scalar_copy(step):
        return pltpu.make_async_remote_copy(
            src_ref=part, dst_ref=parts.at[me], send_sem=ssend, recv_sem=srecv,
            device_id=peer_id(step), device_id_type=MESH,
        )

    @pl.loop(1, count)
    def _(step):
        scalar_copy(step).start()

    @pl.loop(0, 3)
    def _(c):
        for e in range(layers):
            at = pl.ds(e * PTS, PTS)
            fr = flux[0, c, at].reshape(PTS * rows, cols)
            fs = flux[1, c, at].reshape(PTS * rows, cols)
            ft = flux[2, c, at]
            x = along_x(split(fr), tx_ref[...]) + along_y(split(fs), ty_ref[0], ty_ref[1])
            z = jnp.stack(along_z([ft[k] for k in range(PTS)], d.T))
            field[c, at] = assemble_xy(x + z.reshape(x.shape)).reshape(PTS, rows, cols)
        finish_channel(c)

    here = (ix, iy, iz)

    def there(off):
        ok = None
        for o, i, n in zip(off, here, sizes):
            if o:
                t = (i > 0) if o < 0 else (i < n - 1)
                ok = t if ok is None else ok & t
        return ok

    def side(o):
        return (o + 1) // 2

    def copy_to(off):
        n = OFFS.index(off)
        opp = tuple(-o for o in off)
        slot = OFFS.index(opp)
        if off[0]:
            src, dst = pack.at[side(off[0])], rpack.at[XOFF.index(opp)]
        elif off[1] and off[2]:
            src, dst = yzrow.at[side(off[1]), side(off[2])], ryz.at[YZOFF.index(opp)]
        elif off[1]:
            src, dst = yface.at[side(off[1])], ryface.at[YOFF.index(opp)]
        else:
            plane = 0 if off[2] < 0 else planes - 1
            src, dst = field.at[:, plane], rzface.at[ZOFF.index(opp)]
        return pltpu.make_async_remote_copy(
            src_ref=src, dst_ref=dst, send_sem=send_sem.at[n], recv_sem=recv_sem.at[slot],
            device_id={a: i + o for a, i, o in zip(AXES, here, off)}, device_id_type=MESH,
        )

    for off in OFFS:
        @pl.when(there(off))
        def _(off=off):
            copy_to(off).start()

    for off in OFFS:
        @pl.when(there(off))
        def _(off=off):
            n = OFFS.index(off)
            if off[0]:
                dst = rpack.at[XOFF.index(off)]
            elif off[1] and off[2]:
                dst = ryz.at[YZOFF.index(off)]
            elif off[1]:
                dst = ryface.at[YOFF.index(off)]
            else:
                dst = rzface.at[ZOFF.index(off)]
            pltpu.make_async_copy(dst, dst, recv_sem.at[n]).wait()

    pshape = (PTS, cols)
    plane_lane = lax.broadcasted_iota(jnp.int32, pshape, 1)
    prow = lax.broadcasted_iota(jnp.int32, pshape, 0)
    pz = (plane_lane % half) // yel
    pye = plane_lane % yel
    halo = [[None, None], [None, None]]
    for s, dx in ((0, -1), (1, 1)):
        for pair in range(2):
            acc = jnp.zeros(pshape, jnp.float32)
            for off in XOFF:
                if off[0] != dx:
                    continue
                x = rpack[XOFF.index(off), pair]
                keep = None
                shift = 0
                if off[1]:
                    x = pltpu.roll(x, 1 if off[1] < 0 else PTS - 1, 0)
                    keep = ((prow == 0) & (pye == 0)) if off[1] < 0 else ((prow == ORDER) & (pye == yel - 1))
                    shift += -(yel - 1) if off[1] < 0 else yel - 1
                if off[2]:
                    t = (pz == 0) if off[2] < 0 else (pz == planes - 1)
                    keep = t if keep is None else keep & t
                    shift += (-(planes - 1) if off[2] < 0 else planes - 1) * yel
                if shift:
                    x = pltpu.roll(x, shift % cols, 1)
                ok = there(off)
                keep = jnp.broadcast_to(ok, pshape) if keep is None else keep & ok
                acc = acc + jnp.where(keep, x, 0.0)
            halo[s][pair] = acc
    for s in range(2):
        for pair in range(2):
            pack_halo = halo[s][pair]
            flux[0, 0, s * 2 + pair, 0:PTS, :] = pack_halo

    def y_halo(c, s, dy):
        acc = jnp.where(there((0, dy, 0)), ryface[YOFF.index((0, dy, 0)), c], 0.0)
        z1 = lax.broadcasted_iota(jnp.int32, (planes, cols), 0)
        for dz, z in ((-1, 0), (1, planes - 1)):
            off = (0, dy, dz)
            acc = acc + jnp.where((z1 == z) & there(off), ryz[YZOFF.index(off), c], 0.0)
        return acc

    edge = ((lane == 0) & (ix == 0)) | ((lane == cols - 1) & (ix == nx - 1))
    edge = edge | ((k_at == 0) & (ye_at == 0) & (iy == 0))
    edge = edge | ((k_at == ORDER) & (ye_at == yel - 1) & (iy == ny - 1))

    def full(c, store):
        pair, base = c // 2, (c % 2) * half
        ylo = y_halo(c, 0, -1)
        yhi = y_halo(c, 1, 1)
        low = flux[0, 0, pair, 0:PTS, :]
        high = flux[0, 0, 2 + pair, 0:PTS, :]
        for e in range(layers):
            at = pl.ds(e * PTS, PTS)
            hit = lane == base + (e * PTS + z_at) * yel + ye_at
            wide = jnp.concatenate(
                [
                    jnp.where(hit, high[None, None], 0.0).reshape(PTS * rows, cols),
                    jnp.where(hit, low[None, None], 0.0).reshape(PTS * rows, cols),
                ],
                axis=1,
            )
            hi, lo = split(wide)
            x = (dot(hi, put_ref[...]) + dot(lo, put_ref[...])).reshape(four)
            x = x + field[c, at].reshape(four)
            yl = ylo[e * PTS:(e + 1) * PTS][:, None, None, :]
            yh = yhi[e * PTS:(e + 1) * PTS][:, None, None, :]
            x = x + jnp.where((k_at == 0) & (ye_at == 0), yl, 0.0)
            x = x + jnp.where((k_at == ORDER) & (ye_at == yel - 1), yh, 0.0)
            out_edge = edge
            if e == 0:
                zl = jnp.where(there((0, 0, -1)), rzface[0, c], 0.0).reshape(1, yel, PTS, cols)
                x = x + jnp.where(z_at == 0, zl, 0.0)
                out_edge = out_edge | ((z_at == 0) & (iz == 0))
            if e == layers - 1:
                zh = jnp.where(there((0, 0, 1)), rzface[1, c], 0.0).reshape(1, yel, PTS, cols)
                x = x + jnp.where(z_at == PTS - 1, zh, 0.0)
                out_edge = out_edge | ((z_at == PTS - 1) & (iz == nz - 1))
            store(at, jnp.where(out_edge, 0.0, x).reshape(PTS, rows, cols))

    def store_mass(at, x):
        m_out[at] = x

    full(3, store_mass)

    @pl.loop(0, 3)
    def _(c):
        def store(at, x):
            a_out[c, at] = x

        full(c, store)

    rest = parts.at[pl.ds(0, count - 1)]
    pltpu.make_async_copy(rest, rest, srecv).wait()
    total = jnp.sum(parts[...], axis=0)
    total = jnp.sum(total, axis=1, keepdims=True)
    s_out[0:2, :] = jnp.broadcast_to(total, (2, cols))
    s_out[2:3, :] = jnp.broadcast_to(total[1:2] / (2.0 * total[0:1]), (1, cols))

    for off in OFFS:
        @pl.when(there(off))
        def _(off=off):
            copy_to(off).wait_send()

    @pl.loop(1, count)
    def _(step):
        scalar_copy(step).wait_send()


def per_device(sizes, velocity, geometry, mass_weights):
    planes, rows, cols = mass_weights.shape
    f32 = jnp.float32
    count = sizes[0] * sizes[1] * sizes[2]
    vmem = pl.BlockSpec(memory_space=pltpu.VMEM)
    hbm = pl.BlockSpec(memory_space=pl.ANY)
    applied, mass, scalars = pl.pallas_call(
        functools.partial(kernel, sizes),
        out_shape=(
            jax.ShapeDtypeStruct(velocity.shape, f32),
            jax.ShapeDtypeStruct(mass_weights.shape, f32),
            jax.ShapeDtypeStruct((8, cols), f32),
        ),
        in_specs=[hbm] * 3 + [vmem] * 6,
        out_specs=(vmem, vmem, vmem),
        scratch_shapes=[
            pltpu.VMEM(velocity.shape, f32),
            pltpu.VMEM(geometry.shape, geometry.dtype),
            pltpu.VMEM(mass_weights.shape, mass_weights.dtype),
            pltpu.VMEM((3,) + velocity.shape, f32),
            pltpu.VMEM((4, planes, rows, cols), f32),
            pltpu.VMEM((2, 2, PTS, cols), f32),
            pltpu.VMEM((2, 4, planes, cols), f32),
            pltpu.VMEM((2, 2, 4, 1, cols), f32),
            pltpu.VMEM((len(XOFF), 2, PTS, cols), f32),
            pltpu.VMEM((2, 4, planes, cols), f32),
            pltpu.VMEM((2, 4, rows, cols), f32),
            pltpu.VMEM((len(YZOFF), 4, 1, cols), f32),
            pltpu.VMEM((2, cols), f32),
            pltpu.VMEM((count, 2, cols), f32),
            pltpu.SemaphoreType.DMA((3,)),
            pltpu.SemaphoreType.DMA((len(OFFS),)),
            pltpu.SemaphoreType.DMA((len(OFFS),)),
            pltpu.SemaphoreType.DMA,
            pltpu.SemaphoreType.DMA,
        ],
        compiler_params=pltpu.CompilerParams(
            collective_id=0, has_side_effects=True, vmem_limit_bytes=40 * 1024 * 1024
        ),
    )(velocity, geometry, mass_weights, *tables(rows, cols))
    residual = applied - scalars[2, 0] * mass[None] * velocity
    return residual, scalars[0, 0], scalars[1, 0]


def solution(mesh):
    sizes = tuple(mesh.shape[a] for a in AXES)
    in_specs = (P(None, "gz", "gy", "gx"), P(None, "gz", "gy", "gx"), P("gz", "gy", "gx"))
    out_specs = (P(None, "gz", "gy", "gx"), P(), P())
    return jax.shard_map(
        functools.partial(per_device, sizes),
        mesh=mesh, in_specs=in_specs, out_specs=out_specs, check_vma=False,
    )
```

```python
import functools
import itertools

import jax
import jax.numpy as jnp
import numpy as np
from jax import lax
from jax.experimental import pallas as pl
from jax.experimental.pallas import tpu as pltpu
from jax.sharding import PartitionSpec as P

ORDER = 7
PTS = ORDER + 1
MESH = pl.DeviceIdType.MESH
AXES = ("gx", "gy", "gz")
XOFF = [o for o in itertools.product((-1, 0, 1), repeat=3) if o[0] != 0]
YZOFF = [o for o in itertools.product((-1, 0, 1), repeat=3) if o[0] == 0 and o[1] != 0 and o[2] != 0]
YOFF = [(0, -1, 0), (0, 1, 0)]
ZOFF = [(0, 0, -1), (0, 0, 1)]
OFFS = sorted(XOFF + YZOFF + YOFF + ZOFF, key=lambda o: -sum(map(abs, o)))


def gll_derivative(poly_order):
    node_count = poly_order + 1
    abscissa = np.cos(np.pi * np.arange(node_count) / poly_order)
    legendre = np.zeros((node_count, node_count))
    for newton_step in range(60):
        legendre[:, 0] = 1.0
        legendre[:, 1] = abscissa
        for degree in range(2, node_count):
            legendre[:, degree] = (
                (2 * degree - 1) * abscissa * legendre[:, degree - 1]
                - (degree - 1) * legendre[:, degree - 2]
            ) / degree
        abscissa = abscissa - (abscissa * legendre[:, poly_order] - legendre[:, poly_order - 1]) / (
            node_count * legendre[:, poly_order]
        )
    abscissa = abscissa[::-1]
    end_values = legendre[::-1, poly_order]
    spacing = abscissa[:, None] - abscissa[None, :] + np.eye(node_count)
    deriv_table = end_values[:, None] / end_values[None, :] / spacing
    deriv_table = deriv_table * (1.0 - np.eye(node_count))
    deriv_table[0, 0] = -poly_order * node_count / 4.0
    deriv_table[poly_order, poly_order] = poly_order * node_count / 4.0
    return deriv_table.astype(np.float32)


def split_np(m):
    hi = m.astype(jnp.bfloat16)
    lo = (m - hi.astype(np.float32)).astype(jnp.bfloat16)
    return hi, lo


def tables(rows, cols):
    d = gll_derivative(ORDER)
    out = []
    for mat in (d, d.T):
        hi, lo = split_np(np.kron(np.eye(cols // PTS, dtype=np.float32), mat.T))
        zero = np.zeros_like(lo)
        out.append(np.block([[hi, lo], [hi, zero]]))
        hi, lo = split_np(np.kron(np.eye(PTS * rows // PTS, dtype=np.float32), mat))
        out.append(np.stack([hi, lo]))
    pick = np.zeros((2 * cols, 2 * cols), np.float32)
    for base in (0, cols):
        pick[base, :cols] = 1.0
        pick[base + cols - 1, cols:] = 1.0
    out.append(pick.astype(jnp.bfloat16))
    put = np.zeros((2 * cols, cols), np.float32)
    put[:cols, cols - 1] = 1.0
    put[cols:, 0] = 1.0
    out.append(put.astype(jnp.bfloat16))
    return [jnp.asarray(t) for t in out]


def split(x):
    hi = x.astype(jnp.bfloat16)
    lo = (x - hi.astype(jnp.float32)).astype(jnp.bfloat16)
    return hi, lo


def dot(a, b):
    return jnp.dot(a, b, preferred_element_type=jnp.float32)


def along_x(pair, table):
    cols = table.shape[1] // 2
    r = dot(jnp.concatenate(pair, axis=1), table)
    return r[:, :cols] + r[:, cols:]


def along_y(pair, hi, lo):
    cols = pair[0].shape[1]
    r = dot(hi, jnp.concatenate(pair, axis=1))
    return r[:, :cols] + r[:, cols:] + dot(lo, pair[0])


def along_z(planes, mat):
    out = []
    for w in range(PTS):
        acc = planes[0] * float(mat[w, 0])
        for z in range(1, PTS):
            acc = acc + planes[z] * float(mat[w, z])
        out.append(acc)
    return out


def kernel(
    sizes,
    v_hbm, g_hbm, m_hbm, dx_hbm, dy_hbm, tx_hbm, ty_hbm, pick_hbm, put_hbm,
    a_out, b_out, s_out,
    v, g, m, dx_ref, dy_ref, tx_ref, ty_ref, pick_ref, put_ref, mfull, flux, field, pack, yface, yzrow, rpack, ryface, rzface, ryz, part, parts,
    in_sem, send_sem, recv_sem, ssend, srecv,
):
    nx, ny, nz = sizes
    count = nx * ny * nz
    planes, rows, cols = v.shape[1:]
    layers = planes // PTS
    yel = rows // PTS
    half = cols // 2
    ix, iy, iz = (lax.axis_index(a) for a in AXES)
    me = (ix * ny + iy) * nz + iz
    d = gll_derivative(ORDER)

    loads = [
        pltpu.make_async_copy(src, dst, in_sem.at[k])
        for k, (src, dst) in enumerate(
            (
                (m_hbm, m), (pick_hbm, pick_ref), (v_hbm, v), (g_hbm, g), (dx_hbm, dx_ref),
                (dy_hbm, dy_ref), (tx_hbm, tx_ref), (ty_hbm, ty_ref), (put_hbm, put_ref),
            )
        )
    ]
    for c in loads:
        c.start()

    def peer_id(step):
        p = lax.rem(me + step, count)
        return {"gx": p // (ny * nz), "gy": lax.rem(p // nz, ny), "gz": lax.rem(p, nz)}

    barrier = pltpu.get_barrier_semaphore()

    @pl.loop(1, count)
    def _(step):
        pl.semaphore_signal(barrier, inc=1, device_id=peer_id(step), device_id_type=MESH)

    four = (PTS, yel, PTS, cols)
    ye_at = lax.broadcasted_iota(jnp.int32, four, 1)
    k_at = lax.broadcasted_iota(jnp.int32, four, 2)
    z_at = lax.broadcasted_iota(jnp.int32, four, 0)
    lane = lax.broadcasted_iota(jnp.int32, four, 3)
    lane2 = lax.broadcasted_iota(jnp.int32, (PTS * rows, cols), 1)
    row2 = lax.broadcasted_iota(jnp.int32, (PTS * rows, cols), 0)

    def assemble_xy(x):
        n = PTS * rows
        x = (
            x
            + jnp.where((lane2 % PTS == ORDER) & (lane2 < cols - 1), pltpu.roll(x, cols - 1, 1), 0.0)
            + jnp.where((lane2 % PTS == 0) & (lane2 > 0), pltpu.roll(x, 1, 1), 0.0)
        )
        return (
            x
            + jnp.where((row2 % PTS == ORDER) & (row2 % rows < rows - 1), pltpu.roll(x, n - 1, 0), 0.0)
            + jnp.where((row2 % PTS == 0) & (row2 % rows > 0), pltpu.roll(x, 1, 0), 0.0)
        )

    def finish_channel(c):
        for e in range(1, layers):
            low = field[c, e * PTS - 1]
            high = field[c, e * PTS]
            both = low + high
            field[c, e * PTS - 1] = both
            field[c, e * PTS] = both
        lo_acc = jnp.zeros((PTS, cols), jnp.float32)
        hi_acc = jnp.zeros((PTS, cols), jnp.float32)
        base = (c % 2) * half
        for e in range(layers):
            x = field[c, pl.ds(e * PTS, PTS)].reshape(PTS * rows, cols)
            r = dot(jnp.concatenate(split(x), axis=1), pick_ref[...])
            hit = lane == base + (e * PTS + z_at) * yel + ye_at
            lo_acc = lo_acc + jnp.sum(jnp.where(hit, r[:, :cols].reshape(four), 0.0), axis=(0, 1))
            hi_acc = hi_acc + jnp.sum(jnp.where(hit, r[:, cols:].reshape(four), 0.0), axis=(0, 1))
        pair = c // 2
        pack[0, pair] = pack[0, pair] + lo_acc
        pack[1, pair] = pack[1, pair] + hi_acc
        for side, y in ((0, 0), (1, rows - 1)):
            face = field[c, :, y, :]
            yface[side, c] = face
            yzrow[side, 0, c] = face[0:1]
            yzrow[side, 1, c] = face[planes - 1:planes]

    pack[...] = jnp.zeros(pack.shape, jnp.float32)
    loads[0].wait()
    loads[1].wait()
    for e in range(layers):
        x = m[pl.ds(e * PTS, PTS)].astype(jnp.float32).reshape(PTS * rows, cols)
        field[3, pl.ds(e * PTS, PTS)] = assemble_xy(x).reshape(PTS, rows, cols)
    finish_channel(3)
    for c in loads[2:]:
        c.wait()

    def gradients(step, acc):
        kin, ens = acc
        c = step // layers
        at = pl.ds(pl.multiple_of((step % layers) * PTS, PTS), PTS)
        block = v[c, at]
        flat = block.reshape(PTS * rows, cols)
        mass = m[at].astype(jnp.float32)
        kin = kin + jnp.sum((mass * block * block).reshape(-1, PTS, cols), axis=0)
        pair = split(flat)
        gr = along_x(pair, dx_ref[...]).reshape(block.shape)
        gs = along_y(pair, dy_ref[0], dy_ref[1]).reshape(block.shape)
        gt = jnp.stack(along_z([block[z] for z in range(PTS)], d))
        g0, g1, g2, g3, g4, g5 = (g[k, at].astype(jnp.float32) for k in range(6))
        fr = g0 * gr + g3 * gs + g4 * gt
        fs = g3 * gr + g1 * gs + g5 * gt
        ft = g4 * gr + g5 * gs + g2 * gt
        ens = ens + jnp.sum((gr * fr + gs * fs + gt * ft).reshape(-1, PTS, cols), axis=0)
        flux[0, c, at] = fr
        flux[1, c, at] = fs
        flux[2, c, at] = ft
        return kin, ens

    zero = jnp.zeros((PTS, cols), jnp.float32)
    kin, ens = lax.fori_loop(0, 3 * layers, gradients, (zero, zero))
    mine = jnp.concatenate(
        [jnp.sum(kin, 0, keepdims=True) * 0.5, jnp.sum(ens, 0, keepdims=True)], axis=0
    )
    part[...] = mine
    parts[me] = mine

    pl.semaphore_wait(barrier, count - 1)

    def scalar_copy(step):
        return pltpu.make_async_remote_copy(
            src_ref=part, dst_ref=parts.at[me], send_sem=ssend, recv_sem=srecv,
            device_id=peer_id(step), device_id_type=MESH,
        )

    @pl.loop(1, count)
    def _(step):
        scalar_copy(step).start()

    @pl.loop(0, 3)
    def _(c):
        for e in range(layers):
            at = pl.ds(e * PTS, PTS)
            fr = flux[0, c, at].reshape(PTS * rows, cols)
            fs = flux[1, c, at].reshape(PTS * rows, cols)
            ft = flux[2, c, at]
            x = along_x(split(fr), tx_ref[...]) + along_y(split(fs), ty_ref[0], ty_ref[1])
            z = jnp.stack(along_z([ft[k] for k in range(PTS)], d.T))
            field[c, at] = assemble_xy(x + z.reshape(x.shape)).reshape(PTS, rows, cols)
        finish_channel(c)

    here = (ix, iy, iz)

    def there(off):
        ok = None
        for o, i, n in zip(off, here, sizes):
            if o:
                t = (i > 0) if o < 0 else (i < n - 1)
                ok = t if ok is None else ok & t
        return ok

    def side(o):
        return (o + 1) // 2

    def copy_to(off):
        n = OFFS.index(off)
        opp = tuple(-o for o in off)
        slot = OFFS.index(opp)
        if off[0]:
            src, dst = pack.at[side(off[0])], rpack.at[XOFF.index(opp)]
        elif off[1] and off[2]:
            src, dst = yzrow.at[side(off[1]), side(off[2])], ryz.at[YZOFF.index(opp)]
        elif off[1]:
            src, dst = yface.at[side(off[1])], ryface.at[YOFF.index(opp)]
        else:
            plane = 0 if off[2] < 0 else planes - 1
            src, dst = field.at[:, plane], rzface.at[ZOFF.index(opp)]
        return pltpu.make_async_remote_copy(
            src_ref=src, dst_ref=dst, send_sem=send_sem.at[n], recv_sem=recv_sem.at[slot],
            device_id={a: i + o for a, i, o in zip(AXES, here, off)}, device_id_type=MESH,
        )

    for off in OFFS:
        @pl.when(there(off))
        def _(off=off):
            copy_to(off).start()

    for off in OFFS:
        @pl.when(there(off))
        def _(off=off):
            n = OFFS.index(off)
            if off[0]:
                dst = rpack.at[XOFF.index(off)]
            elif off[1] and off[2]:
                dst = ryz.at[YZOFF.index(off)]
            elif off[1]:
                dst = ryface.at[YOFF.index(off)]
            else:
                dst = rzface.at[ZOFF.index(off)]
            pltpu.make_async_copy(dst, dst, recv_sem.at[n]).wait()

    pshape = (PTS, cols)
    plane_lane = lax.broadcasted_iota(jnp.int32, pshape, 1)
    prow = lax.broadcasted_iota(jnp.int32, pshape, 0)
    pz = (plane_lane % half) // yel
    pye = plane_lane % yel
    halo = [[None, None], [None, None]]
    for s, dx in ((0, -1), (1, 1)):
        for pair in range(2):
            acc = jnp.zeros(pshape, jnp.float32)
            for off in XOFF:
                if off[0] != dx:
                    continue
                x = rpack[XOFF.index(off), pair]
                keep = None
                shift = 0
                if off[1]:
                    x = pltpu.roll(x, 1 if off[1] < 0 else PTS - 1, 0)
                    keep = ((prow == 0) & (pye == 0)) if off[1] < 0 else ((prow == ORDER) & (pye == yel - 1))
                    shift += -(yel - 1) if off[1] < 0 else yel - 1
                if off[2]:
                    t = (pz == 0) if off[2] < 0 else (pz == planes - 1)
                    keep = t if keep is None else keep & t
                    shift += (-(planes - 1) if off[2] < 0 else planes - 1) * yel
                if shift:
                    x = pltpu.roll(x, shift % cols, 1)
                ok = there(off)
                keep = jnp.broadcast_to(ok, pshape) if keep is None else keep & ok
                acc = acc + jnp.where(keep, x, 0.0)
            halo[s][pair] = acc
    for s in range(2):
        for pair in range(2):
            pack_halo = halo[s][pair]
            flux[0, 0, s * 2 + pair, 0:PTS, :] = pack_halo

    def y_halo(c, s, dy):
        acc = jnp.where(there((0, dy, 0)), ryface[YOFF.index((0, dy, 0)), c], 0.0)
        z1 = lax.broadcasted_iota(jnp.int32, (planes, cols), 0)
        for dz, z in ((-1, 0), (1, planes - 1)):
            off = (0, dy, dz)
            acc = acc + jnp.where((z1 == z) & there(off), ryz[YZOFF.index(off), c], 0.0)
        return acc

    edge = ((lane == 0) & (ix == 0)) | ((lane == cols - 1) & (ix == nx - 1))
    edge = edge | ((k_at == 0) & (ye_at == 0) & (iy == 0))
    edge = edge | ((k_at == ORDER) & (ye_at == yel - 1) & (iy == ny - 1))

    def full(c, store):
        pair, base = c // 2, (c % 2) * half
        ylo = y_halo(c, 0, -1)
        yhi = y_halo(c, 1, 1)
        low = flux[0, 0, pair, 0:PTS, :]
        high = flux[0, 0, 2 + pair, 0:PTS, :]
        for e in range(layers):
            at = pl.ds(e * PTS, PTS)
            hit = lane == base + (e * PTS + z_at) * yel + ye_at
            wide = jnp.concatenate(
                [
                    jnp.where(hit, high[None, None], 0.0).reshape(PTS * rows, cols),
                    jnp.where(hit, low[None, None], 0.0).reshape(PTS * rows, cols),
                ],
                axis=1,
            )
            hi, lo = split(wide)
            x = (dot(hi, put_ref[...]) + dot(lo, put_ref[...])).reshape(four)
            x = x + field[c, at].reshape(four)
            yl = ylo[e * PTS:(e + 1) * PTS][:, None, None, :]
            yh = yhi[e * PTS:(e + 1) * PTS][:, None, None, :]
            x = x + jnp.where((k_at == 0) & (ye_at == 0), yl, 0.0)
            x = x + jnp.where((k_at == ORDER) & (ye_at == yel - 1), yh, 0.0)
            out_edge = edge
            if e == 0:
                zl = jnp.where(there((0, 0, -1)), rzface[0, c], 0.0).reshape(1, yel, PTS, cols)
                x = x + jnp.where(z_at == 0, zl, 0.0)
                out_edge = out_edge | ((z_at == 0) & (iz == 0))
            if e == layers - 1:
                zh = jnp.where(there((0, 0, 1)), rzface[1, c], 0.0).reshape(1, yel, PTS, cols)
                x = x + jnp.where(z_at == PTS - 1, zh, 0.0)
                out_edge = out_edge | ((z_at == PTS - 1) & (iz == nz - 1))
            store(at, jnp.where(out_edge, 0.0, x).reshape(PTS, rows, cols))

    def store_mass(at, x):
        mfull[at] = x

    full(3, store_mass)

    @pl.loop(0, 3)
    def _(c):
        def store(at, x):
            a_out[c, at] = x
            b_out[c, at] = mfull[at] * v[c, at]

        full(c, store)

    rest = parts.at[pl.ds(0, count - 1)]
    pltpu.make_async_copy(rest, rest, srecv).wait()
    total = jnp.sum(parts[...], axis=0)
    total = jnp.sum(total, axis=1, keepdims=True)
    s_out[...] = jnp.broadcast_to(total, (2, cols))

    for off in OFFS:
        @pl.when(there(off))
        def _(off=off):
            copy_to(off).wait_send()

    @pl.loop(1, count)
    def _(step):
        scalar_copy(step).wait_send()


def finish(a_ref, b_ref, s_ref, r_hbm, k_hbm, e_hbm, r, k, e, sem):
    chunks = r.shape[0]
    kin = s_ref[0:1, 0:1]
    ens = s_ref[1:2, 0:1]
    rayleigh = ens / (2.0 * kin)
    k[...] = kin
    e[...] = ens
    outs = [
        pltpu.make_async_copy(k, k_hbm, sem.at[chunks]),
        pltpu.make_async_copy(e, e_hbm, sem.at[chunks + 1]),
    ]
    for c in range(chunks):
        r[c] = a_ref[c] - rayleigh[None] * b_ref[c]
        outs.append(pltpu.make_async_copy(r.at[c], r_hbm.at[c], sem.at[c]))
        outs[-1].start()
    outs[0].start()
    outs[1].start()
    for c in outs:
        c.wait()


def per_device(sizes, velocity, geometry, mass_weights):
    planes, rows, cols = mass_weights.shape
    f32 = jnp.float32
    count = sizes[0] * sizes[1] * sizes[2]
    vmem = pl.BlockSpec(memory_space=pltpu.VMEM)
    hbm = pl.BlockSpec(memory_space=pltpu.HBM)
    consts = tables(rows, cols)
    applied, weighted, scalars = pl.pallas_call(
        functools.partial(kernel, sizes),
        out_shape=(
            jax.ShapeDtypeStruct(velocity.shape, f32),
            jax.ShapeDtypeStruct(velocity.shape, f32),
            jax.ShapeDtypeStruct((2, cols), f32),
        ),
        in_specs=[hbm] * 9,
        out_specs=(vmem, vmem, vmem),
        scratch_shapes=[
            pltpu.VMEM(velocity.shape, f32),
            pltpu.VMEM(geometry.shape, geometry.dtype),
            pltpu.VMEM(mass_weights.shape, mass_weights.dtype),
            *[pltpu.VMEM(t.shape, t.dtype) for t in consts],
            pltpu.VMEM(mass_weights.shape, f32),
            pltpu.VMEM((3,) + velocity.shape, f32),
            pltpu.VMEM((4, planes, rows, cols), f32),
            pltpu.VMEM((2, 2, PTS, cols), f32),
            pltpu.VMEM((2, 4, planes, cols), f32),
            pltpu.VMEM((2, 2, 4, 1, cols), f32),
            pltpu.VMEM((len(XOFF), 2, PTS, cols), f32),
            pltpu.VMEM((2, 4, planes, cols), f32),
            pltpu.VMEM((2, 4, rows, cols), f32),
            pltpu.VMEM((len(YZOFF), 4, 1, cols), f32),
            pltpu.VMEM((2, cols), f32),
            pltpu.VMEM((count, 2, cols), f32),
            pltpu.SemaphoreType.DMA((9,)),
            pltpu.SemaphoreType.DMA((len(OFFS),)),
            pltpu.SemaphoreType.DMA((len(OFFS),)),
            pltpu.SemaphoreType.DMA,
            pltpu.SemaphoreType.DMA,
        ],
        compiler_params=pltpu.CompilerParams(
            collective_id=0, has_side_effects=True, vmem_limit_bytes=32 * 1024 * 1024
        ),
    )(*(pltpu.with_memory_space_constraint(t, pltpu.HBM) for t in (velocity, geometry, mass_weights, *consts)))
    one = jax.ShapeDtypeStruct((1, 1), f32)
    residual, kinetic, enstrophy = pl.pallas_call(
        finish,
        out_shape=(jax.ShapeDtypeStruct(velocity.shape, f32), one, one),
        in_specs=[vmem] * 3,
        out_specs=(hbm,) * 3,
        scratch_shapes=[
            pltpu.VMEM(velocity.shape, f32),
            pltpu.VMEM((1, 1), f32),
            pltpu.VMEM((1, 1), f32),
            pltpu.SemaphoreType.DMA((velocity.shape[0] + 2,)),
        ],
        compiler_params=pltpu.CompilerParams(vmem_limit_bytes=8 * 1024 * 1024),
    )(applied, weighted, scalars)
    return residual, kinetic[0, 0], enstrophy[0, 0]


def solution(mesh):
    sizes = tuple(mesh.shape[a] for a in AXES)
    in_specs = (P(None, "gz", "gy", "gx"), P(None, "gz", "gy", "gx"), P("gz", "gy", "gx"))
    out_specs = (P(None, "gz", "gy", "gx"), P(), P())
    return jax.shard_map(
        functools.partial(per_device, sizes),
        mesh=mesh, in_specs=in_specs, out_specs=out_specs, check_vma=False,
    )
```

```python
import functools
import itertools

import jax
import jax.numpy as jnp
import numpy as np
from jax import lax
from jax.experimental import pallas as pl
from jax.experimental.pallas import tpu as pltpu
from jax.sharding import PartitionSpec as P

ORDER = 7
PTS = ORDER + 1
MESH = pl.DeviceIdType.MESH
AXES = ("gx", "gy", "gz")
XOFF = [o for o in itertools.product((-1, 0, 1), repeat=3) if o[0] != 0]
YZOFF = [o for o in itertools.product((-1, 0, 1), repeat=3) if o[0] == 0 and o[1] != 0 and o[2] != 0]
YOFF = [(0, -1, 0), (0, 1, 0)]
ZOFF = [(0, 0, -1), (0, 0, 1)]
OFFS = sorted(XOFF + YZOFF + YOFF + ZOFF, key=lambda o: -sum(map(abs, o)))


def gll_derivative(poly_order):
    node_count = poly_order + 1
    abscissa = np.cos(np.pi * np.arange(node_count) / poly_order)
    legendre = np.zeros((node_count, node_count))
    for newton_step in range(60):
        legendre[:, 0] = 1.0
        legendre[:, 1] = abscissa
        for degree in range(2, node_count):
            legendre[:, degree] = (
                (2 * degree - 1) * abscissa * legendre[:, degree - 1]
                - (degree - 1) * legendre[:, degree - 2]
            ) / degree
        abscissa = abscissa - (abscissa * legendre[:, poly_order] - legendre[:, poly_order - 1]) / (
            node_count * legendre[:, poly_order]
        )
    abscissa = abscissa[::-1]
    end_values = legendre[::-1, poly_order]
    spacing = abscissa[:, None] - abscissa[None, :] + np.eye(node_count)
    deriv_table = end_values[:, None] / end_values[None, :] / spacing
    deriv_table = deriv_table * (1.0 - np.eye(node_count))
    deriv_table[0, 0] = -poly_order * node_count / 4.0
    deriv_table[poly_order, poly_order] = poly_order * node_count / 4.0
    return deriv_table.astype(np.float32)


def split_np(m):
    hi = m.astype(jnp.bfloat16)
    lo = (m - hi.astype(np.float32)).astype(jnp.bfloat16)
    return hi, lo


def tables(rows, cols):
    d = gll_derivative(ORDER)
    out = []
    for mat in (d, d.T):
        hi, lo = split_np(np.kron(np.eye(cols // PTS, dtype=np.float32), mat.T))
        zero = np.zeros_like(lo)
        out.append(np.block([[hi, lo], [hi, zero]]))
        hi, lo = split_np(np.kron(np.eye(PTS * rows // PTS, dtype=np.float32), mat))
        out.append(np.stack([hi, lo]))
    pick = np.zeros((2 * PTS, 2 * cols), np.float32)
    pick[0, [0, cols]] = 1.0
    pick[1, [cols - 1, 2 * cols - 1]] = 1.0
    out.append(pick.astype(jnp.bfloat16))
    put = np.zeros((16, 4 * cols), np.float32)
    for c in range(4):
        for base in (0, 8):
            put[base + c, c * cols + cols - 1] = 1.0
            put[base + 4 + c, c * cols] = 1.0
    out.append(put.astype(jnp.bfloat16))
    return [jnp.asarray(t) for t in out]


def split(x):
    hi = x.astype(jnp.bfloat16)
    lo = (x - hi.astype(jnp.float32)).astype(jnp.bfloat16)
    return hi, lo


def dot(a, b):
    return jnp.dot(a, b, preferred_element_type=jnp.float32)


def along_x(pair, table):
    cols = table.shape[1] // 2
    r = dot(jnp.concatenate(pair, axis=1), table)
    return r[:, :cols] + r[:, cols:]


def along_y(pair, hi, lo):
    cols = pair[0].shape[1]
    r = dot(hi, jnp.concatenate(pair, axis=1))
    return r[:, :cols] + r[:, cols:] + dot(lo, pair[0])


def along_z(planes, mat):
    n = PTS // 2
    mat = mat.astype(np.float64)
    odd = [planes[j] - planes[ORDER - j] for j in range(n)]
    even = [planes[j] + planes[ORDER - j] for j in range(n)]
    low, high = [], []
    for i in range(n):
        p = q = None
        for j in range(n):
            t = odd[j] * float(0.5 * (mat[i, j] - mat[i, ORDER - j]))
            u = even[j] * float(0.5 * (mat[i, j] + mat[i, ORDER - j]))
            p = t if p is None else p + t
            q = u if q is None else q + u
        low.append(p + q)
        high.append(p - q)
    return low + high[::-1]


def kernel(
    sizes,
    v_hbm, g_hbm, m_hbm, dx_hbm, dy_hbm, tx_hbm, ty_hbm, pick_hbm, put_hbm,
    a_out, b_out, s_out,
    v, g, m, dx_ref, dy_ref, tx_ref, ty_ref, pick_ref, put_ref, flux, field, pack, yface, yzrow, rpack, ryface, rzface, ryz, part, parts, zface, keep, halo,
    in_sem, send_sem, recv_sem, ssend, srecv,
):
    nx, ny, nz = sizes
    count = nx * ny * nz
    planes, rows, cols = v.shape[1:]
    layers = planes // PTS
    yel = rows // PTS
    half = cols // 2
    ix, iy, iz = (lax.axis_index(a) for a in AXES)
    me = (ix * ny + iy) * nz + iz
    d = gll_derivative(ORDER)

    loads = [
        pltpu.make_async_copy(src, dst, in_sem.at[k])
        for k, (src, dst) in enumerate(
            (
                (m_hbm, m), (pick_hbm, pick_ref), (v_hbm, v), (g_hbm, g), (dx_hbm, dx_ref),
                (dy_hbm, dy_ref), (tx_hbm, tx_ref), (ty_hbm, ty_ref), (put_hbm, put_ref),
            )
        )
    ]
    for c in loads:
        c.start()

    def peer_id(step):
        p = lax.rem(me + step, count)
        return {"gx": p // (ny * nz), "gy": lax.rem(p // nz, ny), "gz": lax.rem(p, nz)}

    barrier = pltpu.get_barrier_semaphore()

    @pl.loop(1, count)
    def _(step):
        pl.semaphore_signal(barrier, inc=1, device_id=peer_id(step), device_id_type=MESH)

    n_rows = PTS * rows
    four = (PTS, yel, PTS, cols)
    flat8 = (1, 1, PTS, cols)
    lane = lax.broadcasted_iota(jnp.int32, flat8, 3)
    k_at = lax.broadcasted_iota(jnp.int32, flat8, 2)

    def unit(mask):
        return jnp.where(mask, 1.0, 0.0).astype(jnp.float32)

    x_next = unit((lane % PTS == ORDER) & (lane < cols - 1))
    x_prev = unit((lane % PTS == 0) & (lane > 0))
    y_last = unit(k_at == ORDER)
    y_first = unit(k_at == 0)

    def assemble_xy(x):
        up = pltpu.roll(x, cols - 1, 1).reshape(four)
        down = pltpu.roll(x, 1, 1).reshape(four)
        x = x.reshape(four) + up * x_next + down * x_prev
        flat = x.reshape(PTS * yel, PTS, cols)
        up = pltpu.roll(flat, PTS - 1, 1).reshape(four)
        down = pltpu.roll(flat, 1, 1).reshape(four)
        out = []
        for y in range(yel):
            t = x[:, y:y + 1]
            if y < yel - 1:
                t = t + up[:, y + 1:y + 2] * y_last
            if y > 0:
                t = t + down[:, y - 1:y] * y_first
            out.append(t)
        return jnp.concatenate(out, axis=1).reshape(PTS, rows, cols)

    def finish_channel(c):
        for e in range(1, layers):
            low = field[c, e * PTS - 1]
            high = field[c, e * PTS]
            both = low + high
            field[c, e * PTS - 1] = both
            field[c, e * PTS] = both
        for e in range(layers):
            x = field[c, pl.ds(e * PTS, PTS)].reshape(n_rows, cols)
            r = lax.dot_general(
                pick_ref[...], jnp.concatenate(split(x), axis=1), (((1,), (1,)), ((), ())),
                preferred_element_type=jnp.float32,
            )
            for s in range(2):
                pack[s, pl.ds(c, 1), pl.ds(e * n_rows, n_rows)] = r[s:s + 1]
        for side, y in ((0, 0), (1, rows - 1)):
            face = field[c, :, y, :]
            yface[side, c] = face
            yzrow[side, 0, c] = face[0:1]
            yzrow[side, 1, c] = face[planes - 1:planes]
        zface[0, c] = field[c, 0]
        zface[1, c] = field[c, planes - 1]

    inner_x = unit(((lane > 0) | (ix > 0)) & ((lane < cols - 1) | (ix < nx - 1))).reshape(1, PTS, cols)
    z3 = lax.broadcasted_iota(jnp.int32, (planes, 1, cols), 0)
    inner_z = unit(((z3 > 0) | (iz > 0)) & ((z3 < planes - 1) | (iz < nz - 1)))
    for y in range(yel):
        w = inner_x
        if y == 0:
            w = w * unit((k_at > 0) | (iy > 0)).reshape(1, PTS, cols)
        if y == yel - 1:
            w = w * unit((k_at < ORDER) | (iy < ny - 1)).reshape(1, PTS, cols)
        keep[:, y * PTS:(y + 1) * PTS, :] = w * inner_z
    loads[0].wait()
    loads[1].wait()
    for e in range(layers):
        x = m[pl.ds(e * PTS, PTS)].astype(jnp.float32).reshape(PTS * rows, cols)
        field[3, pl.ds(e * PTS, PTS)] = assemble_xy(x)
    finish_channel(3)
    for c in loads[2:]:
        c.wait()

    def gradients(step, acc):
        kin, ens = acc
        c = step // layers
        at = pl.ds(pl.multiple_of((step % layers) * PTS, PTS), PTS)
        block = v[c, at]
        flat = block.reshape(PTS * rows, cols)
        mass = m[at].astype(jnp.float32)
        kin = kin + jnp.sum((mass * block * block).reshape(-1, PTS, cols), axis=0)
        pair = split(flat)
        gr = along_x(pair, dx_ref[...]).reshape(block.shape)
        gs = along_y(pair, dy_ref[0], dy_ref[1]).reshape(block.shape)
        gt = jnp.stack(along_z([block[z] for z in range(PTS)], d))
        g0, g1, g2, g3, g4, g5 = (g[k, at].astype(jnp.float32) for k in range(6))
        fr = g0 * gr + g3 * gs + g4 * gt
        fs = g3 * gr + g1 * gs + g5 * gt
        ft = g4 * gr + g5 * gs + g2 * gt
        ens = ens + jnp.sum((gr * fr + gs * fs + gt * ft).reshape(-1, PTS, cols), axis=0)
        flux[0, c, at] = fr
        flux[1, c, at] = fs
        flux[2, c, at] = ft
        return kin, ens

    zero = jnp.zeros((PTS, cols), jnp.float32)
    kin, ens = lax.fori_loop(0, 3 * layers, gradients, (zero, zero))
    mine = jnp.concatenate(
        [jnp.sum(kin, 0, keepdims=True) * 0.5, jnp.sum(ens, 0, keepdims=True)], axis=0
    )
    part[...] = mine
    parts[me] = mine

    pl.semaphore_wait(barrier, count - 1)

    def scalar_copy(step):
        return pltpu.make_async_remote_copy(
            src_ref=part, dst_ref=parts.at[me], send_sem=ssend, recv_sem=srecv,
            device_id=peer_id(step), device_id_type=MESH,
        )

    @pl.loop(1, count)
    def _(step):
        scalar_copy(step).start()

    @pl.loop(0, 3)
    def _(c):
        for e in range(layers):
            at = pl.ds(e * PTS, PTS)
            fr = flux[0, c, at].reshape(PTS * rows, cols)
            fs = flux[1, c, at].reshape(PTS * rows, cols)
            ft = flux[2, c, at]
            x = along_x(split(fr), tx_ref[...]) + along_y(split(fs), ty_ref[0], ty_ref[1])
            z = jnp.stack(along_z([ft[k] for k in range(PTS)], d.T))
            field[c, at] = assemble_xy(x + z.reshape(x.shape))
        finish_channel(c)

    here = (ix, iy, iz)

    def there(off):
        ok = None
        for o, i, n in zip(off, here, sizes):
            if o:
                t = (i > 0) if o < 0 else (i < n - 1)
                ok = t if ok is None else ok & t
        return ok

    def side(o):
        return (o + 1) // 2

    def copy_to(off):
        n = OFFS.index(off)
        opp = tuple(-o for o in off)
        slot = OFFS.index(opp)
        if off[0]:
            src, dst = pack.at[side(off[0])], rpack.at[XOFF.index(opp)]
        elif off[1] and off[2]:
            src, dst = yzrow.at[side(off[1]), side(off[2])], ryz.at[YZOFF.index(opp)]
        elif off[1]:
            src, dst = yface.at[side(off[1])], ryface.at[YOFF.index(opp)]
        else:
            src, dst = zface.at[side(off[2])], rzface.at[ZOFF.index(opp)]
        return pltpu.make_async_remote_copy(
            src_ref=src, dst_ref=dst, send_sem=send_sem.at[n], recv_sem=recv_sem.at[slot],
            device_id={a: i + o for a, i, o in zip(AXES, here, off)}, device_id_type=MESH,
        )

    for off in OFFS:
        @pl.when(there(off))
        def _(off=off):
            copy_to(off).start()

    for off in OFFS:
        @pl.when(there(off))
        def _(off=off):
            n = OFFS.index(off)
            if off[0]:
                dst = rpack.at[XOFF.index(off)]
            elif off[1] and off[2]:
                dst = ryz.at[YZOFF.index(off)]
            elif off[1]:
                dst = ryface.at[YOFF.index(off)]
            else:
                dst = rzface.at[ZOFF.index(off)]
            pltpu.make_async_copy(dst, dst, recv_sem.at[n]).wait()

    total_rows = planes * rows
    pshape = (4, total_rows)
    place = lax.broadcasted_iota(jnp.int32, (1, total_rows), 1)
    for s, dx in ((0, 1), (1, -1)):
        acc = jnp.zeros(pshape, jnp.float32)
        for off in XOFF:
            if off[0] != dx:
                continue
            x = rpack[XOFF.index(off)]
            hit = place >= 0
            shift = 0
            if off[1]:
                hit = hit & (place % rows == (0 if off[1] < 0 else rows - 1))
                shift += off[1] * (rows - 1)
            if off[2]:
                hit = hit & (place // rows == (0 if off[2] < 0 else planes - 1))
                shift += off[2] * (planes - 1) * rows
            if shift:
                x = pltpu.roll(x, shift % total_rows, 1)
            acc = acc + jnp.where(jnp.broadcast_to(hit & there(off), pshape), x, 0.0)
        hi, lo = split(acc)
        halo[s * 4:s * 4 + 4, :] = hi.astype(jnp.float32)
        halo[8 + s * 4:12 + s * 4, :] = lo.astype(jnp.float32)

    z1 = lax.broadcasted_iota(jnp.int32, (planes, cols), 0)

    def add_yz(c):
        for dy, y in ((-1, 0), (1, rows - 1)):
            acc = jnp.where(there((0, dy, 0)), ryface[YOFF.index((0, dy, 0)), c], 0.0)
            for dz, z in ((-1, 0), (1, planes - 1)):
                off = (0, dy, dz)
                acc = acc + jnp.where((z1 == z) & there(off), ryz[YZOFF.index(off), c], 0.0)
            field[c, :, y, :] = field[c, :, y, :] + acc
        for k, (dz, z) in enumerate(((-1, 0), (1, planes - 1))):
            field[c, z] = field[c, z] + jnp.where(there((0, 0, dz)), rzface[k, c], 0.0)

    for c in range(4):
        add_yz(c)
    halos = halo[...].astype(jnp.bfloat16)
    for e in range(layers):
        at = pl.ds(e * PTS, PTS)
        x = lax.dot_general(
            halos[:, e * n_rows:(e + 1) * n_rows], put_ref[...], (((0,), (0,)), ((), ())),
            preferred_element_type=jnp.float32,
        )
        w = keep[at]
        mass = (field[3, at] + x[:, 3 * cols:].reshape(PTS, rows, cols)) * w
        for c in range(3):
            a_out[c, at] = (field[c, at] + x[:, c * cols:(c + 1) * cols].reshape(PTS, rows, cols)) * w
            b_out[c, at] = mass * v[c, at]

    rest = parts.at[pl.ds(0, count - 1)]
    pltpu.make_async_copy(rest, rest, srecv).wait()
    total = jnp.sum(parts[...], axis=0)
    total = jnp.sum(total, axis=1, keepdims=True)
    s_out[...] = jnp.broadcast_to(total, (2, cols))

    for off in OFFS:
        @pl.when(there(off))
        def _(off=off):
            copy_to(off).wait_send()

    @pl.loop(1, count)
    def _(step):
        scalar_copy(step).wait_send()


def finish(a_ref, b_ref, s_ref, r_hbm, k_hbm, e_hbm, r, k, e, sem):
    chunks = r.shape[0]
    kin = s_ref[0:1, 0:1]
    ens = s_ref[1:2, 0:1]
    rayleigh = ens / (2.0 * kin)
    k[...] = kin
    e[...] = ens
    outs = [
        pltpu.make_async_copy(k, k_hbm, sem.at[chunks]),
        pltpu.make_async_copy(e, e_hbm, sem.at[chunks + 1]),
    ]
    for c in range(chunks):
        r[c] = a_ref[c] - rayleigh[None] * b_ref[c]
        outs.append(pltpu.make_async_copy(r.at[c], r_hbm.at[c], sem.at[c]))
        outs[-1].start()
    outs[0].start()
    outs[1].start()
    for c in outs:
        c.wait()


def per_device(sizes, velocity, geometry, mass_weights):
    planes, rows, cols = mass_weights.shape
    f32 = jnp.float32
    count = sizes[0] * sizes[1] * sizes[2]
    vmem = pl.BlockSpec(memory_space=pltpu.VMEM)
    hbm = pl.BlockSpec(memory_space=pltpu.HBM)
    consts = tables(rows, cols)
    applied, weighted, scalars = pl.pallas_call(
        functools.partial(kernel, sizes),
        out_shape=(
            jax.ShapeDtypeStruct(velocity.shape, f32),
            jax.ShapeDtypeStruct(velocity.shape, f32),
            jax.ShapeDtypeStruct((2, cols), f32),
        ),
        in_specs=[hbm] * 9,
        out_specs=(vmem, vmem, vmem),
        scratch_shapes=[
            pltpu.VMEM(velocity.shape, f32),
            pltpu.VMEM(geometry.shape, geometry.dtype),
            pltpu.VMEM(mass_weights.shape, mass_weights.dtype),
            *[pltpu.VMEM(t.shape, t.dtype) for t in consts],
            pltpu.VMEM((3,) + velocity.shape, f32),
            pltpu.VMEM((4, planes, rows, cols), f32),
            pltpu.VMEM((2, 4, planes * rows), f32),
            pltpu.VMEM((2, 4, planes, cols), f32),
            pltpu.VMEM((2, 2, 4, 1, cols), f32),
            pltpu.VMEM((len(XOFF), 4, planes * rows), f32),
            pltpu.VMEM((2, 4, planes, cols), f32),
            pltpu.VMEM((2, 4, rows, cols), f32),
            pltpu.VMEM((len(YZOFF), 4, 1, cols), f32),
            pltpu.VMEM((2, cols), f32),
            pltpu.VMEM((count, 2, cols), f32),
            pltpu.VMEM((2, 4, rows, cols), f32),
            pltpu.VMEM(mass_weights.shape, f32),
            pltpu.VMEM((16, planes * rows), f32),
            pltpu.SemaphoreType.DMA((9,)),
            pltpu.SemaphoreType.DMA((len(OFFS),)),
            pltpu.SemaphoreType.DMA((len(OFFS),)),
            pltpu.SemaphoreType.DMA,
            pltpu.SemaphoreType.DMA,
        ],
        compiler_params=pltpu.CompilerParams(
            collective_id=0, has_side_effects=True, vmem_limit_bytes=32 * 1024 * 1024
        ),
    )(*(pltpu.with_memory_space_constraint(t, pltpu.HBM) for t in (velocity, geometry, mass_weights, *consts)))
    one = jax.ShapeDtypeStruct((1, 1), f32)
    residual, kinetic, enstrophy = pl.pallas_call(
        finish,
        out_shape=(jax.ShapeDtypeStruct(velocity.shape, f32), one, one),
        in_specs=[vmem] * 3,
        out_specs=(hbm,) * 3,
        scratch_shapes=[
            pltpu.VMEM(velocity.shape, f32),
            pltpu.VMEM((1, 1), f32),
            pltpu.VMEM((1, 1), f32),
            pltpu.SemaphoreType.DMA((velocity.shape[0] + 2,)),
        ],
        compiler_params=pltpu.CompilerParams(vmem_limit_bytes=8 * 1024 * 1024),
    )(applied, weighted, scalars)
    return residual, kinetic[0, 0], enstrophy[0, 0]


def solution(mesh):
    sizes = tuple(mesh.shape[a] for a in AXES)
    in_specs = (P(None, "gz", "gy", "gx"), P(None, "gz", "gy", "gx"), P("gz", "gy", "gx"))
    out_specs = (P(None, "gz", "gy", "gx"), P(), P())
    return jax.shard_map(
        functools.partial(per_device, sizes),
        mesh=mesh, in_specs=in_specs, out_specs=out_specs, check_vma=False,
    )
```

```python
import functools
import itertools

import jax
import jax.numpy as jnp
import numpy as np
from jax import lax
from jax.experimental import pallas as pl
from jax.experimental.pallas import tpu as pltpu
from jax.sharding import PartitionSpec as P

ORDER = 7
PTS = ORDER + 1
MESH = pl.DeviceIdType.MESH
AXES = ("gx", "gy", "gz")
XOFF = [o for o in itertools.product((-1, 0, 1), repeat=3) if o[0] != 0]
YZOFF = [o for o in itertools.product((-1, 0, 1), repeat=3) if o[0] == 0 and o[1] != 0 and o[2] != 0]
YOFF = [(0, -1, 0), (0, 1, 0)]
FACES = YOFF + [(0, 0, -1), (0, 0, 1)]
OFFS = sorted(XOFF + YZOFF, key=lambda o: -sum(map(abs, o)))


def gll_derivative(poly_order):
    node_count = poly_order + 1
    abscissa = np.cos(np.pi * np.arange(node_count) / poly_order)
    legendre = np.zeros((node_count, node_count))
    for newton_step in range(60):
        legendre[:, 0] = 1.0
        legendre[:, 1] = abscissa
        for degree in range(2, node_count):
            legendre[:, degree] = (
                (2 * degree - 1) * abscissa * legendre[:, degree - 1]
                - (degree - 1) * legendre[:, degree - 2]
            ) / degree
        abscissa = abscissa - (abscissa * legendre[:, poly_order] - legendre[:, poly_order - 1]) / (
            node_count * legendre[:, poly_order]
        )
    abscissa = abscissa[::-1]
    end_values = legendre[::-1, poly_order]
    spacing = abscissa[:, None] - abscissa[None, :] + np.eye(node_count)
    deriv_table = end_values[:, None] / end_values[None, :] / spacing
    deriv_table = deriv_table * (1.0 - np.eye(node_count))
    deriv_table[0, 0] = -poly_order * node_count / 4.0
    deriv_table[poly_order, poly_order] = poly_order * node_count / 4.0
    return deriv_table.astype(np.float32)


def split_np(m):
    hi = m.astype(jnp.bfloat16)
    lo = (m - hi.astype(np.float32)).astype(jnp.bfloat16)
    return hi, lo


def tables(rows, cols):
    d = gll_derivative(ORDER)
    out = []
    for mat in (d, d.T):
        hi, lo = split_np(np.kron(np.eye(cols // PTS, dtype=np.float32), mat.T))
        zero = np.zeros_like(lo)
        out.append(np.block([[hi, lo], [hi, zero]]))
        hi, lo = split_np(np.kron(np.eye(PTS * rows // PTS, dtype=np.float32), mat))
        out.append(np.stack([hi, lo]))
    pick = np.zeros((2 * PTS, 2 * cols), np.float32)
    pick[0, [0, cols]] = 1.0
    pick[1, [cols - 1, 2 * cols - 1]] = 1.0
    out.append(pick.astype(jnp.bfloat16))
    put = np.zeros((16, 4 * cols), np.float32)
    for c in range(4):
        for base in (0, 8):
            put[base + c, c * cols + cols - 1] = 1.0
            put[base + 4 + c, c * cols] = 1.0
    out.append(put.astype(jnp.bfloat16))
    return [jnp.asarray(t) for t in out]


def split(x):
    hi = x.astype(jnp.bfloat16)
    lo = (x - hi.astype(jnp.float32)).astype(jnp.bfloat16)
    return hi, lo


def dot(a, b):
    return jnp.dot(a, b, preferred_element_type=jnp.float32)


def along_x(pair, table):
    cols = table.shape[1] // 2
    r = dot(jnp.concatenate(pair, axis=1), table)
    return r[:, :cols] + r[:, cols:]


def along_y(pair, hi, lo):
    cols = pair[0].shape[1]
    r = dot(hi, jnp.concatenate(pair, axis=1))
    return r[:, :cols] + r[:, cols:] + dot(lo, pair[0])


def along_z(planes, mat):
    n = PTS // 2
    mat = mat.astype(np.float64)
    odd = [planes[j] - planes[ORDER - j] for j in range(n)]
    even = [planes[j] + planes[ORDER - j] for j in range(n)]
    low, high = [], []
    for i in range(n):
        p = q = None
        for j in range(n):
            t = odd[j] * float(0.5 * (mat[i, j] - mat[i, ORDER - j]))
            u = even[j] * float(0.5 * (mat[i, j] + mat[i, ORDER - j]))
            p = t if p is None else p + t
            q = u if q is None else q + u
        low.append(p + q)
        high.append(p - q)
    return low + high[::-1]


def kernel(
    sizes,
    v_hbm, g_hbm, m_hbm, dx_hbm, dy_hbm, tx_hbm, ty_hbm, pick_hbm, put_hbm,
    a_out, b_out, s_out,
    v, g, m, dx_ref, dy_ref, tx_ref, ty_ref, pick_ref, put_ref, flux, field, pack, yface, yzrow, rpack, ryface, rzface, ryz, part, parts, zface, keep, halo,
    in_sem, send_sem, recv_sem, ssend, srecv, fsend, frecv,
):
    nx, ny, nz = sizes
    count = nx * ny * nz
    planes, rows, cols = v.shape[1:]
    layers = planes // PTS
    yel = rows // PTS
    half = cols // 2
    ix, iy, iz = (lax.axis_index(a) for a in AXES)
    me = (ix * ny + iy) * nz + iz
    d = gll_derivative(ORDER)

    loads = [
        pltpu.make_async_copy(src, dst, in_sem.at[k])
        for k, (src, dst) in enumerate(
            (
                (m_hbm, m), (pick_hbm, pick_ref), (v_hbm, v), (g_hbm, g), (dx_hbm, dx_ref),
                (dy_hbm, dy_ref), (tx_hbm, tx_ref), (ty_hbm, ty_ref), (put_hbm, put_ref),
            )
        )
    ]
    for c in loads:
        c.start()

    def peer_id(step):
        p = lax.rem(me + step, count)
        return {"gx": p // (ny * nz), "gy": lax.rem(p // nz, ny), "gz": lax.rem(p, nz)}

    def ring(i, n):
        out = [i]
        for _ in range(n - 1):
            t = out[-1] + 1
            out.append(jnp.where(t == n, 0, t))
        return out

    def for_peers(act):
        if count > 64:
            pl.loop(1, count)(lambda step: act(peer_id(step)))
            return
        xs, ys, zs = (ring(i, n) for i, n in zip((ix, iy, iz), sizes))
        for x, y, z in itertools.product(range(nx), range(ny), range(nz)):
            if x or y or z:
                act({"gx": xs[x], "gy": ys[y], "gz": zs[z]})

    barrier = pltpu.get_barrier_semaphore()
    for_peers(
        lambda to: pl.semaphore_signal(barrier, inc=1, device_id=to, device_id_type=MESH)
    )

    n_rows = PTS * rows
    four = (PTS, yel, PTS, cols)
    flat8 = (1, 1, PTS, cols)
    lane = lax.broadcasted_iota(jnp.int32, flat8, 3)
    k_at = lax.broadcasted_iota(jnp.int32, flat8, 2)

    def unit(mask):
        return jnp.where(mask, 1.0, 0.0).astype(jnp.float32)

    x_next = unit((lane % PTS == ORDER) & (lane < cols - 1))
    x_prev = unit((lane % PTS == 0) & (lane > 0))
    y_last = unit(k_at == ORDER)
    y_first = unit(k_at == 0)

    def assemble_xy(x):
        up = pltpu.roll(x, cols - 1, 1).reshape(four)
        down = pltpu.roll(x, 1, 1).reshape(four)
        x = x.reshape(four) + up * x_next + down * x_prev
        flat = x.reshape(PTS * yel, PTS, cols)
        up = pltpu.roll(flat, PTS - 1, 1).reshape(four)
        down = pltpu.roll(flat, 1, 1).reshape(four)
        out = []
        for y in range(yel):
            t = x[:, y:y + 1]
            if y < yel - 1:
                t = t + up[:, y + 1:y + 2] * y_last
            if y > 0:
                t = t + down[:, y - 1:y] * y_first
            out.append(t)
        return jnp.concatenate(out, axis=1).reshape(PTS, rows, cols)

    def finish_channel(c):
        for e in range(1, layers):
            low = field[c, e * PTS - 1]
            high = field[c, e * PTS]
            both = low + high
            field[c, e * PTS - 1] = both
            field[c, e * PTS] = both
        for e in range(layers):
            x = field[c, pl.ds(e * PTS, PTS)].reshape(n_rows, cols)
            r = lax.dot_general(
                pick_ref[...], jnp.concatenate(split(x), axis=1), (((1,), (1,)), ((), ())),
                preferred_element_type=jnp.float32,
            )
            for s in range(2):
                pack[s, pl.ds(c, 1), pl.ds(e * n_rows, n_rows)] = r[s:s + 1]
        for side, y in ((0, 0), (1, rows - 1)):
            face = field[c, :, y, :]
            yface[side, c] = face
            yzrow[side, 0, c] = face[0:1]
            yzrow[side, 1, c] = face[planes - 1:planes]
        zface[0, c] = field[c, 0]
        zface[1, c] = field[c, planes - 1]

    total_rows = planes * rows
    here = (ix, iy, iz)

    def there(off):
        ok = None
        for o, i, n in zip(off, here, sizes):
            if o:
                t = (i > 0) if o < 0 else (i < n - 1)
                ok = t if ok is None else ok & t
        return ok

    def side(o):
        return (o + 1) // 2

    def target(off):
        return {a: i + o for a, i, o in zip(AXES, here, off)}

    def part_of(dz):
        width = total_rows // layers // 2
        width = width if width % 128 == 0 else total_rows
        if dz == 0:
            return pl.ds(0, total_rows)
        return pl.ds(0 if dz < 0 else total_rows - width, width)

    def landing(off):
        if off[0]:
            return rpack.at[XOFF.index(off), :, part_of(-off[2])]
        return ryz.at[YZOFF.index(off)]

    def copy_to(off):
        opp = tuple(-o for o in off)
        if off[0]:
            src = pack.at[side(off[0]), :, part_of(off[2])]
        else:
            src = yzrow.at[side(off[1]), side(off[2])]
        return pltpu.make_async_remote_copy(
            src_ref=src, dst_ref=landing(opp), send_sem=send_sem.at[OFFS.index(off)],
            recv_sem=recv_sem.at[OFFS.index(opp)], device_id=target(off), device_id_type=MESH,
        )

    def face_copy(off, c):
        k, opp = FACES.index(off), FACES.index(tuple(-o for o in off))
        src, dst = (yface, ryface) if off[1] else (zface, rzface)
        return pltpu.make_async_remote_copy(
            src_ref=src.at[k % 2, c], dst_ref=dst.at[opp % 2, c], send_sem=fsend.at[k, c],
            recv_sem=frecv.at[opp, c], device_id=target(off), device_id_type=MESH,
        )

    def send_faces(c):
        for off in FACES[::-1]:
            @pl.when(there(off))
            def _(off=off):
                face_copy(off, c).start()

    inner_x = unit(((lane > 0) | (ix > 0)) & ((lane < cols - 1) | (ix < nx - 1))).reshape(1, PTS, cols)
    z3 = lax.broadcasted_iota(jnp.int32, (planes, 1, cols), 0)
    inner_z = unit(((z3 > 0) | (iz > 0)) & ((z3 < planes - 1) | (iz < nz - 1)))
    for y in range(yel):
        w = inner_x
        if y == 0:
            w = w * unit((k_at > 0) | (iy > 0)).reshape(1, PTS, cols)
        if y == yel - 1:
            w = w * unit((k_at < ORDER) | (iy < ny - 1)).reshape(1, PTS, cols)
        keep[:, y * PTS:(y + 1) * PTS, :] = w * inner_z
    loads[0].wait()
    loads[1].wait()
    for e in range(layers):
        x = m[pl.ds(e * PTS, PTS)].astype(jnp.float32).reshape(PTS * rows, cols)
        field[3, pl.ds(e * PTS, PTS)] = assemble_xy(x)
    finish_channel(3)
    for c in loads[2:]:
        c.wait()

    def gradients(e, acc):
        kin, ens = acc
        at = pl.ds(pl.multiple_of(e * PTS, PTS), PTS)
        mass = m[at].astype(jnp.float32)
        g0, g1, g2, g3, g4, g5 = (g[k, at].astype(jnp.float32) for k in range(6))
        for c in range(3):
            block = v[c, at]
            flat = block.reshape(PTS * rows, cols)
            kin = kin + jnp.sum((mass * block * block).reshape(-1, PTS, cols), axis=0)
            pair = split(flat)
            gr = along_x(pair, dx_ref[...]).reshape(block.shape)
            gs = along_y(pair, dy_ref[0], dy_ref[1]).reshape(block.shape)
            gt = jnp.stack(along_z([block[z] for z in range(PTS)], d))
            fr = g0 * gr + g3 * gs + g4 * gt
            fs = g3 * gr + g1 * gs + g5 * gt
            ft = g4 * gr + g5 * gs + g2 * gt
            ens = ens + jnp.sum((gr * fr + gs * fs + gt * ft).reshape(-1, PTS, cols), axis=0)
            flux[0, c, at] = fr
            flux[1, c, at] = fs
            flux[2, c, at] = ft
        return kin, ens

    zero = jnp.zeros((PTS, cols), jnp.float32)
    kin, ens = lax.fori_loop(0, layers, gradients, (zero, zero))
    mine = jnp.concatenate(
        [jnp.sum(kin, 0, keepdims=True) * 0.5, jnp.sum(ens, 0, keepdims=True)], axis=0
    )
    part[...] = mine
    parts[me] = mine

    pl.semaphore_wait(barrier, count - 1)

    def scalar_copy(to):
        return pltpu.make_async_remote_copy(
            src_ref=part, dst_ref=parts.at[me], send_sem=ssend, recv_sem=srecv,
            device_id=to, device_id_type=MESH,
        )

    for_peers(lambda to: scalar_copy(to).start())
    send_faces(3)

    @pl.loop(0, 3)
    def _(c):
        for e in range(layers):
            at = pl.ds(e * PTS, PTS)
            fr = flux[0, c, at].reshape(PTS * rows, cols)
            fs = flux[1, c, at].reshape(PTS * rows, cols)
            ft = flux[2, c, at]
            x = along_x(split(fr), tx_ref[...]) + along_y(split(fs), ty_ref[0], ty_ref[1])
            z = jnp.stack(along_z([ft[k] for k in range(PTS)], d.T))
            field[c, at] = assemble_xy(x + z.reshape(x.shape))
        finish_channel(c)
        send_faces(c)

    for off in OFFS:
        @pl.when(there(off))
        def _(off=off):
            copy_to(off).start()

    for off in OFFS:
        @pl.when(there(off))
        def _(off=off):
            dst = landing(off)
            pltpu.make_async_copy(dst, dst, recv_sem.at[OFFS.index(off)]).wait()

    for k, off in enumerate(FACES):
        @pl.when(there(off))
        def _(k=k, off=off):
            for c in range(4):
                dst = (ryface if off[1] else rzface).at[k % 2, c]
                pltpu.make_async_copy(dst, dst, frecv.at[k, c]).wait()

    pshape = (4, total_rows)
    place = lax.broadcasted_iota(jnp.int32, (1, total_rows), 1)
    for s, dx in ((0, 1), (1, -1)):
        acc = jnp.zeros(pshape, jnp.float32)
        for off in XOFF:
            if off[0] != dx:
                continue
            x = rpack[XOFF.index(off)]
            hit = place >= 0
            shift = 0
            if off[1]:
                hit = hit & (place % rows == (0 if off[1] < 0 else rows - 1))
                shift += off[1] * (rows - 1)
            if off[2]:
                hit = hit & (place // rows == (0 if off[2] < 0 else planes - 1))
                shift += off[2] * (planes - 1) * rows
            if shift:
                x = pltpu.roll(x, shift % total_rows, 1)
            acc = acc + jnp.where(jnp.broadcast_to(hit & there(off), pshape), x, 0.0)
        hi, lo = split(acc)
        halo[s * 4:s * 4 + 4, :] = hi.astype(jnp.float32)
        halo[8 + s * 4:12 + s * 4, :] = lo.astype(jnp.float32)

    z1 = lax.broadcasted_iota(jnp.int32, (planes, cols), 0)

    def add_yz(c):
        for dy, y in ((-1, 0), (1, rows - 1)):
            acc = jnp.where(there((0, dy, 0)), ryface[YOFF.index((0, dy, 0)), c], 0.0)
            for dz, z in ((-1, 0), (1, planes - 1)):
                off = (0, dy, dz)
                acc = acc + jnp.where((z1 == z) & there(off), ryz[YZOFF.index(off), c], 0.0)
            field[c, :, y, :] = field[c, :, y, :] + acc
        for k, (dz, z) in enumerate(((-1, 0), (1, planes - 1))):
            field[c, z] = field[c, z] + jnp.where(there((0, 0, dz)), rzface[k, c], 0.0)

    for c in range(4):
        add_yz(c)
    halos = halo[...].astype(jnp.bfloat16)
    for e in range(layers):
        at = pl.ds(e * PTS, PTS)
        x = lax.dot_general(
            halos[:, e * n_rows:(e + 1) * n_rows], put_ref[...], (((0,), (0,)), ((), ())),
            preferred_element_type=jnp.float32,
        )
        w = keep[at]
        mass = (field[3, at] + x[:, 3 * cols:].reshape(PTS, rows, cols)) * w
        for c in range(3):
            a_out[c, at] = (field[c, at] + x[:, c * cols:(c + 1) * cols].reshape(PTS, rows, cols)) * w
            b_out[c, at] = mass * v[c, at]

    rest = parts.at[pl.ds(0, count - 1)]
    pltpu.make_async_copy(rest, rest, srecv).wait()
    total = jnp.sum(parts[...], axis=0)
    total = jnp.sum(total, axis=1, keepdims=True)
    s_out[...] = jnp.broadcast_to(total, (2, cols))

    for off in OFFS:
        @pl.when(there(off))
        def _(off=off):
            copy_to(off).wait_send()

    for off in FACES:
        @pl.when(there(off))
        def _(off=off):
            for c in range(4):
                face_copy(off, c).wait_send()

    sent = parts.at[pl.ds(0, count - 1)]
    pltpu.make_async_copy(sent, sent, ssend).wait()


def finish(a_ref, b_ref, s_ref, r_hbm, k_hbm, e_hbm, r, k, e, sem):
    chunks = r.shape[0]
    kin = s_ref[0:1, 0:1]
    ens = s_ref[1:2, 0:1]
    rayleigh = ens / (2.0 * kin)
    k[...] = kin
    e[...] = ens
    outs = [
        pltpu.make_async_copy(k, k_hbm, sem.at[chunks]),
        pltpu.make_async_copy(e, e_hbm, sem.at[chunks + 1]),
    ]
    for c in range(chunks):
        r[c] = a_ref[c] - rayleigh[None] * b_ref[c]
        outs.append(pltpu.make_async_copy(r.at[c], r_hbm.at[c], sem.at[c]))
        outs[-1].start()
    outs[0].start()
    outs[1].start()
    for c in outs:
        c.wait()


def per_device(sizes, velocity, geometry, mass_weights):
    planes, rows, cols = mass_weights.shape
    f32 = jnp.float32
    count = sizes[0] * sizes[1] * sizes[2]
    vmem = pl.BlockSpec(memory_space=pltpu.VMEM)
    hbm = pl.BlockSpec(memory_space=pltpu.HBM)
    consts = tables(rows, cols)
    applied, weighted, scalars = pl.pallas_call(
        functools.partial(kernel, sizes),
        out_shape=(
            jax.ShapeDtypeStruct(velocity.shape, f32),
            jax.ShapeDtypeStruct(velocity.shape, f32),
            jax.ShapeDtypeStruct((2, cols), f32),
        ),
        in_specs=[hbm] * 9,
        out_specs=(vmem, vmem, vmem),
        scratch_shapes=[
            pltpu.VMEM(velocity.shape, f32),
            pltpu.VMEM(geometry.shape, geometry.dtype),
            pltpu.VMEM(mass_weights.shape, mass_weights.dtype),
            *[pltpu.VMEM(t.shape, t.dtype) for t in consts],
            pltpu.VMEM((3,) + velocity.shape, f32),
            pltpu.VMEM((4, planes, rows, cols), f32),
            pltpu.VMEM((2, 4, planes * rows), f32),
            pltpu.VMEM((2, 4, planes, cols), f32),
            pltpu.VMEM((2, 2, 4, 1, cols), f32),
            pltpu.VMEM((len(XOFF), 4, planes * rows), f32),
            pltpu.VMEM((2, 4, planes, cols), f32),
            pltpu.VMEM((2, 4, rows, cols), f32),
            pltpu.VMEM((len(YZOFF), 4, 1, cols), f32),
            pltpu.VMEM((2, cols), f32),
            pltpu.VMEM((count, 2, cols), f32),
            pltpu.VMEM((2, 4, rows, cols), f32),
            pltpu.VMEM(mass_weights.shape, f32),
            pltpu.VMEM((16, planes * rows), f32),
            pltpu.SemaphoreType.DMA((9,)),
            pltpu.SemaphoreType.DMA((len(OFFS),)),
            pltpu.SemaphoreType.DMA((len(OFFS),)),
            pltpu.SemaphoreType.DMA,
            pltpu.SemaphoreType.DMA,
            pltpu.SemaphoreType.DMA((len(FACES), 4)),
            pltpu.SemaphoreType.DMA((len(FACES), 4)),
        ],
        compiler_params=pltpu.CompilerParams(
            collective_id=0, has_side_effects=True, vmem_limit_bytes=32 * 1024 * 1024
        ),
    )(*(pltpu.with_memory_space_constraint(t, pltpu.HBM) for t in (velocity, geometry, mass_weights, *consts)))
    one = jax.ShapeDtypeStruct((1, 1), f32)
    residual, kinetic, enstrophy = pl.pallas_call(
        finish,
        out_shape=(jax.ShapeDtypeStruct(velocity.shape, f32), one, one),
        in_specs=[vmem] * 3,
        out_specs=(hbm,) * 3,
        scratch_shapes=[
            pltpu.VMEM(velocity.shape, f32),
            pltpu.VMEM((1, 1), f32),
            pltpu.VMEM((1, 1), f32),
            pltpu.SemaphoreType.DMA((velocity.shape[0] + 2,)),
        ],
        compiler_params=pltpu.CompilerParams(vmem_limit_bytes=8 * 1024 * 1024),
    )(applied, weighted, scalars)
    return residual, kinetic[0, 0], enstrophy[0, 0]


def solution(mesh):
    sizes = tuple(mesh.shape[a] for a in AXES)
    in_specs = (P(None, "gz", "gy", "gx"), P(None, "gz", "gy", "gx"), P("gz", "gy", "gx"))
    out_specs = (P(None, "gz", "gy", "gx"), P(), P())
    return jax.shard_map(
        functools.partial(per_device, sizes),
        mesh=mesh, in_specs=in_specs, out_specs=out_specs, check_vma=False,
    )
```
